32 devices in a mesh: row: 8 (over y, x, core), col: 4 (over z).
Axes of the slice: x: 2, y: 2, z: 4, core: 2. Of those that a mesh axis runs over, the one named last changes fastest.
Arguments:
- velocity: float32 [128, 128, 2048], P(None, 'row', 'col'), may hold values from -6 to 6
- symbol_x: float32 [128], replicated, may hold values from 0.3 to 3
- symbol_y: float32 [128], replicated, may hold values from 0.3 to 3
- symbol_z: float32 [2048], replicated, may hold values from 0.3 to 3
Outputs:
- coefficients: float32 [128, 128, 2048], P('row', 'col')
The draws below stay inside these ranges and needn't reach their ends.
All inputs are finite; a program needn't handle non-finite values.
Results may differ from the reference program's by a relative error of at most 0.000076.
Values sent between devices are 32-bit elements; how exact they have to be, the bound alone decides.
A program may use at most 192 MiB of HBM per device.

```python
import jax
import jax.numpy as jnp
from jax import lax

GRID_X = 128
GRID_Y = 128
GRID_Z = 2048


def level_of(own_key, shape, pieces, low, largest):
    factor_of = 1.0
    for dim, shards_of in pieces:
        draws = jax.random.uniform(jax.random.fold_in(jax.random.fold_in(own_key, 6), dim), (shards_of,), jnp.float32, low / len(pieces), largest / len(pieces))
        factor_of = factor_of * jnp.repeat(jnp.exp(draws), shape[dim] // shards_of).reshape((-1,) + (1,) * (len(shape) - 1 - dim))
    return factor_of


def normal_values(stream_key, dims, width, limit, split=(), held_as=jnp.bfloat16):
    drawn = jax.random.normal(stream_key, dims, jnp.float32) * width
    if len(split) > 0:
        drawn = level_of(stream_key, dims, split, -0.22, 0.18) * drawn
    return jnp.clip(drawn, min=-limit, max=limit).astype(held_as)


def setup_inputs(seed: int = 0) -> dict:
    seeds = jax.random.split(jax.random.key(seed), 5)
    velocity = normal_values(seeds[0], (GRID_X, GRID_Y, GRID_Z), 1.0, 6.0, ((1, 8), (2, 4)), jnp.float32)
    symbol_x = jnp.clip(jax.random.uniform(seeds[1], (GRID_X,), jnp.float32, 0.3, 3.0), 0.3, 3.0)
    symbol_y = jnp.clip(jax.random.uniform(seeds[2], (GRID_Y,), jnp.float32, 0.3, 3.0), 0.3, 3.0)
    symbol_z = jnp.clip(jax.random.uniform(seeds[3], (GRID_Z,), jnp.float32, 0.3, 3.0), 0.3, 3.0)
    return {"velocity": velocity, "symbol_x": symbol_x, "symbol_y": symbol_y, "symbol_z": symbol_z}


def mode_table(count):
    rank = jnp.arange(count)
    angle = (2.0 * jnp.pi / count) * ((rank[:, None] * rank[None, :]) % count).astype(jnp.float32)
    return (jnp.cos(angle) + jnp.sin(angle)) * (count ** -0.5)


def along_dim(values, dim):
    moved = jnp.tensordot(values, mode_table(values.shape[dim]), axes=([dim], [0]), precision=lax.Precision.HIGHEST)
    return jnp.moveaxis(moved, -1, dim)


def reference(velocity, symbol_x, symbol_y, symbol_z):
    coefficients = velocity
    coefficients = along_dim(coefficients, 0)
    coefficients = along_dim(coefficients, 1)
    coefficients = along_dim(coefficients, 2)
    symbol = symbol_x[:, None, None] + symbol_y[None, :, None] + symbol_z[None, None, :]
    coefficients = coefficients * ((1.0 - 0.2 * symbol) / (1.0 + 0.2 * symbol))
    return coefficients
```

```python
import functools

import jax
import jax.numpy as jnp
import numpy as np
from jax import lax
from jax.experimental import pallas as pl
from jax.experimental.pallas import tpu as pltpu
from jax.sharding import PartitionSpec as P

SUB = 8
MESH = pl.DeviceIdType.MESH


def mode_table(count):
    rank = jnp.arange(count)
    angle = 2.0 * jnp.pi / count * (rank[:, None] * rank[None, :] % count).astype(jnp.float32)
    return (jnp.cos(angle) + jnp.sin(angle)) * count ** (-0.5)


def along_dim(values, dim):
    moved = jnp.tensordot(
        values, mode_table(values.shape[dim]), axes=([dim], [0]), precision=lax.Precision.HIGHEST
    )
    return jnp.moveaxis(moved, -1, dim)


def fixed_table(count):
    rank = np.arange(count)
    angle = 2.0 * np.pi / count * (rank[:, None] * rank[None, :] % count)
    return ((np.cos(angle) + np.sin(angle)) * count ** (-0.5)).astype(np.float32)


def halves(table):
    high = table.astype(jnp.bfloat16)
    low = (table - high.astype(np.float32)).astype(jnp.bfloat16)
    return high, low


def split(values):
    high = values.astype(jnp.bfloat16)
    low = (values - high.astype(jnp.float32)).astype(jnp.bfloat16)
    return high, low


def product(a, b):
    return jnp.dot(a, b, preferred_element_type=jnp.float32)


def flipped(index, mask):
    out = index
    bit = 1
    while bit <= mask:
        if mask & bit:
            out = out + bit * (1 - 2 * ((index // bit) % 2))
        bit *= 2
    return out


def kernel(
    dims, v_hbm, w_hbm, h_ref, t_hbm, out_ref,
    v, w, t, v_parts, xs, rbuf, ybuf, zbuf, lhs,
    load_sem, row_send, row_recv, col_send, col_recv,
):
    rows, cols, chunks, per, ahead, lag = dims
    part_y, part_z = v.shape[1], v.shape[2]
    grid_x, grid_y = v.shape[0], rbuf.shape[1]
    share_y, grid_z = zbuf.shape[1], zbuf.shape[2]
    tiles, tile = t.shape[1], t.shape[3]
    r, c = lax.axis_index("row"), lax.axis_index("col")

    load_v = pltpu.make_async_copy(v_hbm, v, load_sem.at[0])
    load_w = pltpu.make_async_copy(w_hbm, w, load_sem.at[1])
    load_t = pltpu.make_async_copy(t_hbm, t, load_sem.at[2])
    load_v.start()
    load_w.start()
    load_t.start()

    row_masks = sorted(range(1, rows), key=lambda m: (-bin(m // 2).count("1"), m))
    row_peers = [flipped(r, m) for m in row_masks]
    col_peers = [flipped(c, m) for m in sorted(range(1, cols), reverse=True)]

    barrier = pltpu.get_barrier_semaphore()
    for s in row_peers:
        pl.semaphore_signal(barrier, inc=1, device_id=(s, c), device_id_type=MESH)
    for s in col_peers:
        pl.semaphore_signal(barrier, inc=1, device_id=(r, s), device_id_type=MESH)

    load_v.wait()
    step = SUB * SUB

    def part_loop(i, carry):
        for g in range(part_y // SUB):
            block = v[pl.ds(i * SUB, SUB), g * SUB:(g + 1) * SUB, :].reshape(step, part_z)
            high, low = split(block)
            v_parts[g, 0, pl.ds(pl.multiple_of(i * step, step), step), :] = high
            v_parts[g, 1, pl.ds(pl.multiple_of(i * step, step), step), :] = low
        return carry

    lax.fori_loop(0, grid_x // SUB, part_loop, 0)
    load_w.wait()
    pl.semaphore_wait(barrier, len(row_peers) + len(col_peers))

    def x_stage(k):
        m = w.shape[1] // 2
        for g in range(part_y // SUB):
            both = product(w[k], v_parts[g, 0])
            sums = both[:m] + both[m:] + product(w[k, :m], v_parts[g, 1])
            xs[k, :, g * SUB:(g + 1) * SUB, :] = sums.reshape(rows * per, SUB, part_z)

    def row_stage(k):
        for s in row_peers:
            pltpu.make_async_remote_copy(
                src_ref=xs.at[k, pl.ds(s * per, per)],
                dst_ref=rbuf.at[pl.ds(k * per, per), pl.ds(pl.multiple_of(r * part_y, SUB), part_y), :],
                send_sem=row_send.at[k], recv_sem=row_recv.at[k],
                device_id=(s, c), device_id_type=MESH,
            ).start()
        rbuf[pl.ds(k * per, per), pl.ds(pl.multiple_of(r * part_y, SUB), part_y), :] = xs[k, pl.ds(r * per, per)]

    def row_bytes(k, sem):
        ref = rbuf.at[pl.ds(k * per, per), pl.ds(0, grid_y - part_y), :]
        return pltpu.make_async_copy(ref, ref, sem.at[k])

    def col_bytes(k, sem):
        ref = zbuf.at[pl.ds(k * per, per), :, pl.ds(0, grid_z - part_z)]
        return pltpu.make_async_copy(ref, ref, sem.at[k])

    def y_stage(k):
        row_bytes(k, row_recv).wait()
        for i in range(per):
            high, low = split(rbuf[k * per + i])
            both = product(h_ref[...], high)
            ybuf[k, i] = both[:grid_y] + both[grid_y:] + product(h_ref[:grid_y], low)
        for s in col_peers:
            pltpu.make_async_remote_copy(
                src_ref=ybuf.at[k, :, pl.ds(pl.multiple_of(s * share_y, SUB), share_y), :],
                dst_ref=zbuf.at[pl.ds(k * per, per), :, pl.ds(pl.multiple_of(c * part_z, 128), part_z)],
                send_sem=col_send.at[k], recv_sem=col_recv.at[k],
                device_id=(r, s), device_id_type=MESH,
            ).start()
        zbuf[pl.ds(k * per, per), :, pl.ds(pl.multiple_of(c * part_z, 128), part_z)] = (
            ybuf[k, :, pl.ds(pl.multiple_of(c * share_y, SUB), share_y), :]
        )

    def z_stage(k):
        col_bytes(k, col_recv).wait()
        m = per * share_y
        high, low = split(zbuf[pl.ds(k * per, per)].reshape(m, grid_z))
        lhs[:m] = high
        lhs[m:] = low

        def tile_loop(n, carry):
            both = product(lhs[...], t[0, n])
            sums = both[:m] + both[m:] + product(lhs[:m], t[1, n])
            out_ref[pl.ds(k * per, per), :, pl.ds(pl.multiple_of(n * tile, tile), tile)] = (
                sums.reshape(per, share_y, tile)
            )
            return carry

        lax.fori_loop(0, tiles, tile_loop, 0)

    def loop(k, carry):
        @pl.when(k < chunks)
        def _():
            x_stage(k)
            row_stage(k)

        @pl.when((k >= ahead) & (k < chunks + ahead))
        def _():
            y_stage(k - ahead)

        @pl.when(k == ahead + lag)
        def _():
            load_t.wait()

        @pl.when(k >= ahead + lag)
        def _():
            z_stage(k - ahead - lag)

        return carry

    lax.fori_loop(0, chunks + ahead + lag, loop, 0)

    def drain(k, carry):
        row_bytes(k, row_send).wait()
        col_bytes(k, col_send).wait()
        return carry

    lax.fori_loop(0, chunks, drain, 0)


def transformed(rows, cols, velocity):
    grid_x, part_y, part_z = velocity.shape
    grid_y, grid_z = part_y * rows, part_z * cols
    share_x, share_y = grid_x // rows, grid_y // cols
    chunks = min(8, share_x)
    per = share_x // chunks
    tile = 256
    hx, hy, hz = fixed_table(grid_x), fixed_table(grid_y), fixed_table(grid_z)
    order = np.arange(grid_x).reshape(rows, chunks, per).transpose(1, 0, 2).reshape(chunks, rows * per)
    w = np.stack([np.kron(hx[o], np.eye(SUB, dtype=np.float32)) for o in order])
    w = np.concatenate(halves(w), axis=1)
    h = np.concatenate(halves(hy), axis=0)
    t = np.stack(halves(hz)).reshape(2, grid_z, grid_z // tile, tile).transpose(0, 2, 1, 3)
    f32, bf16 = jnp.float32, jnp.bfloat16
    any_spec = pl.BlockSpec(memory_space=pl.ANY)
    vmem = pl.BlockSpec(memory_space=pltpu.VMEM)
    return pl.pallas_call(
        functools.partial(kernel, (rows, cols, chunks, per, 1, 2)),
        out_shape=jax.ShapeDtypeStruct((share_x, share_y, grid_z), f32),
        in_specs=[any_spec, any_spec, vmem, any_spec],
        out_specs=vmem,
        scratch_shapes=[
            pltpu.VMEM(velocity.shape, f32),
            pltpu.VMEM(w.shape, bf16),
            pltpu.VMEM(t.shape, bf16),
            pltpu.VMEM((part_y // SUB, 2, grid_x * SUB, part_z), bf16),
            pltpu.VMEM((chunks, rows * per, part_y, part_z), f32),
            pltpu.VMEM((share_x, grid_y, part_z), f32),
            pltpu.VMEM((chunks, per, grid_y, part_z), f32),
            pltpu.VMEM((share_x, share_y, grid_z), f32),
            pltpu.VMEM((2 * per * share_y, grid_z), bf16),
            pltpu.SemaphoreType.DMA((3,)),
            pltpu.SemaphoreType.DMA((chunks,)),
            pltpu.SemaphoreType.DMA((chunks,)),
            pltpu.SemaphoreType.DMA((chunks,)),
            pltpu.SemaphoreType.DMA((chunks,)),
        ],
        compiler_params=pltpu.CompilerParams(
            collective_id=0, has_side_effects=True, vmem_limit_bytes=58 * 2**20
        ),
    )(velocity, jnp.asarray(w), jnp.asarray(h), jnp.asarray(np.ascontiguousarray(t)))


def fits(rows, cols, shape):
    grid_x, part_y, part_z = shape
    grid_z = part_z * cols
    held = 7 * grid_x * part_y * part_z * 4 + 4 * grid_z * grid_z + 4 * (grid_x * SUB) ** 2
    even = rows & (rows - 1) == 0 and cols & (cols - 1) == 0 and grid_x % (8 * rows) == 0
    return even and part_y % SUB == 0 and part_z % 128 == 0 and (part_y * rows) % (SUB * cols) == 0 and held < 54 * 2**20


def local(rows, cols, velocity, symbol_x, symbol_y, symbol_z):
    if fits(rows, cols, velocity.shape):
        pencil_values = transformed(rows, cols, velocity)
    else:
        part_values = along_dim(velocity, 0)
        part_values = lax.all_to_all(part_values, "row", split_axis=0, concat_axis=1, tiled=True)
        pencil_values = along_dim(part_values, 1)
        pencil_values = lax.all_to_all(pencil_values, "col", split_axis=1, concat_axis=2, tiled=True)
        pencil_values = along_dim(pencil_values, 2)
    share_x = pencil_values.shape[0]
    part_x = lax.dynamic_slice_in_dim(symbol_x, lax.axis_index("row") * share_x, share_x)
    share_y = pencil_values.shape[1]
    part_y = lax.dynamic_slice_in_dim(symbol_y, lax.axis_index("col") * share_y, share_y)
    symbol = part_x[:, None, None] + part_y[None, :, None] + symbol_z[None, None, :]
    return pencil_values * ((1.0 - 0.2 * symbol) / (1.0 + 0.2 * symbol))


def solution(mesh):
    placed = (P(None, "row", "col"), P(), P(), P())
    return jax.shard_map(
        functools.partial(local, mesh.shape["row"], mesh.shape["col"]),
        mesh=mesh, in_specs=placed, out_specs=P("row", "col", None), check_vma=False,
    )
```

```python
import functools

import jax
import jax.numpy as jnp
import numpy as np
from jax import lax
from jax.experimental import pallas as pl
from jax.experimental.pallas import tpu as pltpu
from jax.sharding import PartitionSpec as P

SUB = 8
MESH = pl.DeviceIdType.MESH


def mode_table(count):
    rank = jnp.arange(count)
    angle = 2.0 * jnp.pi / count * (rank[:, None] * rank[None, :] % count).astype(jnp.float32)
    return (jnp.cos(angle) + jnp.sin(angle)) * count ** (-0.5)


def along_dim(values, dim):
    moved = jnp.tensordot(
        values, mode_table(values.shape[dim]), axes=([dim], [0]), precision=lax.Precision.HIGHEST
    )
    return jnp.moveaxis(moved, -1, dim)


def fixed_table(count):
    rank = np.arange(count)
    angle = 2.0 * np.pi / count * (rank[:, None] * rank[None, :] % count)
    return ((np.cos(angle) + np.sin(angle)) * count ** (-0.5)).astype(np.float32)


def halves(table):
    high = table.astype(jnp.bfloat16)
    low = (table - high.astype(np.float32)).astype(jnp.bfloat16)
    return high, low


def split(values):
    high = values.astype(jnp.bfloat16)
    low = (values - high.astype(jnp.float32)).astype(jnp.bfloat16)
    return high, low


def product(a, b):
    return jnp.dot(a, b, preferred_element_type=jnp.float32)


def flipped(index, mask):
    out = index
    bit = 1
    while bit <= mask:
        if mask & bit:
            out = out + bit * (1 - 2 * ((index // bit) % 2))
        bit *= 2
    return out


def kernel(
    dims, v_hbm, w_hbm, t_hbm, sx_ref, sy_ref, sz_ref, out_ref,
    v, w, t, v_parts, xs, rbuf, ybuf, zbuf, lhs, sx_col, sy_col,
    load_sem, row_send, row_recv, col_send, col_recv,
):
    rows, cols, chunks, per, ahead, lag = dims
    part_y, part_z = v.shape[1], v.shape[2]
    grid_x, grid_y = v.shape[0], rbuf.shape[1]
    share_y, grid_z = zbuf.shape[1], zbuf.shape[2]
    tiles, tile = t.shape[1], t.shape[3]
    r, c = lax.axis_index("row"), lax.axis_index("col")

    load_v = pltpu.make_async_copy(v_hbm, v, load_sem.at[0])
    load_w = pltpu.make_async_copy(w_hbm.at[0], w.at[0], load_sem.at[1])
    load_rest = pltpu.make_async_copy(w_hbm.at[pl.ds(1, chunks - 1)], w.at[pl.ds(1, chunks - 1)], load_sem.at[2])
    load_t = pltpu.make_async_copy(t_hbm, t, load_sem.at[3])
    load_v.start()
    load_w.start()

    row_masks = sorted(range(1, rows), key=lambda m: (-bin(m // 2).count("1"), m))
    row_peers = [flipped(r, m) for m in row_masks]
    col_peers = [flipped(c, m) for m in range(1, cols)]

    barrier = pltpu.get_barrier_semaphore()
    for s in row_peers:
        pl.semaphore_signal(barrier, inc=1, device_id=(s, c), device_id_type=MESH)
    for s in col_peers:
        pl.semaphore_signal(barrier, inc=1, device_id=(r, s), device_id_type=MESH)

    for ref, column in ((sx_ref, sx_col), (sy_ref, sy_col)):
        column[...] = jnp.broadcast_to(ref[...], (128, ref.shape[1])).T
    load_v.wait()
    load_w.wait()
    load_rest.start()
    step = SUB * SUB

    def part_loop(i, carry):
        for g in range(part_y // SUB):
            block = v[pl.ds(i * SUB, SUB), g * SUB:(g + 1) * SUB, :].reshape(step, part_z)
            high, low = split(block)
            v_parts[g, 0, pl.ds(pl.multiple_of(i * step, step), step), :] = high
            v_parts[g, 1, pl.ds(pl.multiple_of(i * step, step), step), :] = low
        return carry

    lax.fori_loop(0, grid_x // SUB, part_loop, 0)
    load_t.start()
    pl.semaphore_wait(barrier, len(row_peers) + len(col_peers))

    def x_stage(k):
        m, depth = rows * per * SUB, grid_x * SUB
        for g in range(part_y // SUB):
            both = product(w[k, :2 * m, :depth], v_parts[g, 0])
            sums = both[:m] + both[m:] + product(w[k, :m, :depth], v_parts[g, 1])
            xs[k, :, g * SUB:(g + 1) * SUB, :] = sums.reshape(rows * per, SUB, part_z)

    def own_rows():
        return pl.ds(pl.multiple_of(r * part_y, SUB), part_y)

    def row_stage(k):
        for i in range(per):
            for s in row_peers:
                pltpu.make_async_remote_copy(
                    src_ref=xs.at[k, s * per + i],
                    dst_ref=rbuf.at[k * per + i, own_rows(), :],
                    send_sem=row_send.at[k], recv_sem=row_recv.at[k, i],
                    device_id=(s, c), device_id_type=MESH,
                ).start()
        rbuf[pl.ds(k * per, per), own_rows(), :] = xs[k, pl.ds(r * per, per)]

    def y_stage(k):
        for i in range(per):
            came = rbuf.at[k * per + i, pl.ds(0, grid_y - part_y), :]
            pltpu.make_async_copy(came, came, row_recv.at[k, i]).wait()
            high, low = split(rbuf[k * per + i])
            both = product(w[0, :2 * grid_y, grid_x * SUB:], high)
            ybuf[k, i] = both[:grid_y] + both[grid_y:] + product(w[0, :grid_y, grid_x * SUB:], low)
            for m, s in enumerate(col_peers):
                pltpu.make_async_remote_copy(
                    src_ref=ybuf.at[k, i, pl.ds(pl.multiple_of(s * share_y, SUB), share_y), :],
                    dst_ref=zbuf.at[k * per + i, :, pl.ds(pl.multiple_of(c * part_z, 128), part_z)],
                    send_sem=col_send.at[k], recv_sem=col_recv.at[k, m],
                    device_id=(r, s), device_id_type=MESH,
                ).start()
        zbuf[pl.ds(k * per, per), :, pl.ds(pl.multiple_of(c * part_z, 128), part_z)] = (
            ybuf[k, :, pl.ds(pl.multiple_of(c * share_y, SUB), share_y), :]
        )

    def col_wait(k, m):
        came = zbuf.at[pl.ds(k * per, per), :, pl.ds(0, part_z)]
        pltpu.make_async_copy(came, came, col_recv.at[k, m]).wait()

    def scaled(k, n, sums):
        y_part = sy_col[pl.ds(pl.multiple_of(c * share_y, SUB), share_y), :]
        z_part = sz_ref[:, pl.ds(pl.multiple_of(n * tile, tile), tile)]
        plane = jnp.concatenate([y_part] * (tile // 128), axis=1) + z_part
        for i in range(per):
            x_part = sx_col[pl.ds(r * chunks * per + k * per + i, 1), :]
            symbol = jnp.concatenate([x_part] * (tile // 128), axis=1) + plane
            factor = (1.0 - 0.2 * symbol) / (1.0 + 0.2 * symbol)
            out_ref[k * per + i, :, pl.ds(pl.multiple_of(n * tile, tile), tile)] = (
                sums[i * share_y:(i + 1) * share_y] * factor
            )

    size = per * share_y

    def z_stage(k):
        for m in range(len(col_peers)):
            col_wait(k, m)
        high, low = split(zbuf[pl.ds(k * per, per)].reshape(size, grid_z))
        lhs[:size] = high
        lhs[size:] = low

        def tile_loop(n, carry):
            both = product(lhs[...], t[0, n])
            scaled(k, n, both[:size] + both[size:] + product(lhs[:size], t[1, n]))
            return carry

        lax.fori_loop(0, tiles, tile_loop, 0)

    def last_z_stage(k):
        for m, s in enumerate([c] + col_peers):
            if m > 0:
                col_wait(k, m - 1)
            span = pl.ds(pl.multiple_of(s * part_z, 128), part_z)
            high, low = split(zbuf[pl.ds(k * per, per), :, span].reshape(size, part_z))
            lhs[:size, :part_z] = high
            lhs[size:, :part_z] = low

            def tile_loop(n, carry):
                both = product(lhs[:, :part_z], t[0, n, span, :])
                sums = both[:size] + both[size:] + product(lhs[:size, :part_z], t[1, n, span, :])
                at = pl.ds(pl.multiple_of(n * tile, tile), tile)
                if m > 0:
                    sums = sums + out_ref[pl.ds(k * per, per), :, at].reshape(size, tile)
                if m < len(col_peers):
                    out_ref[pl.ds(k * per, per), :, at] = sums.reshape(per, share_y, tile)
                else:
                    scaled(k, n, sums)
                return carry

            lax.fori_loop(0, tiles, tile_loop, 0)

    def loop(k, carry):
        @pl.when(k == 1)
        def _():
            load_rest.wait()

        @pl.when(k < chunks)
        def _():
            x_stage(k)
            row_stage(k)

        @pl.when((k >= ahead) & (k < chunks + ahead))
        def _():
            y_stage(k - ahead)

        @pl.when(k == ahead + lag)
        def _():
            load_t.wait()

        @pl.when(k >= ahead + lag)
        def _():
            z_stage(k - ahead - lag)

        return carry

    lax.fori_loop(0, chunks + ahead + lag - 1, loop, 0)
    last_z_stage(chunks - 1)

    def drain(k, carry):
        sent = rbuf.at[pl.ds(k * per, per), pl.ds(0, grid_y - part_y), :]
        pltpu.make_async_copy(sent, sent, row_send.at[k]).wait()
        sent = zbuf.at[pl.ds(k * per, per), :, pl.ds(0, grid_z - part_z)]
        pltpu.make_async_copy(sent, sent, col_send.at[k]).wait()
        return carry

    lax.fori_loop(0, chunks, drain, 0)


def transformed(rows, cols, velocity, symbol_x, symbol_y, symbol_z):
    grid_x, part_y, part_z = velocity.shape
    grid_y, grid_z = part_y * rows, part_z * cols
    share_x, share_y = grid_x // rows, grid_y // cols
    chunks = min(8, share_x)
    per = share_x // chunks
    tile = 256
    hx, hy, hz = fixed_table(grid_x), fixed_table(grid_y), fixed_table(grid_z)
    order = np.arange(grid_x).reshape(rows, chunks, per).transpose(1, 0, 2).reshape(chunks, rows * per)
    w = np.stack([np.kron(hx[o], np.eye(SUB, dtype=np.float32)) for o in order])
    w = np.concatenate(halves(w), axis=1)
    h = np.concatenate(halves(hy), axis=0)
    t = np.stack(halves(hz)).reshape(2, grid_z, grid_z // tile, tile).transpose(0, 2, 1, 3)
    held = np.zeros((chunks, max(w.shape[1], h.shape[0]), w.shape[2] + h.shape[1]), w.dtype)
    held[:, :w.shape[1], :w.shape[2]] = w
    held[0, :h.shape[0], w.shape[2]:] = h
    f32, bf16 = jnp.float32, jnp.bfloat16
    hbm = pl.BlockSpec(memory_space=pltpu.HBM)
    vmem = pl.BlockSpec(memory_space=pltpu.VMEM)
    return pl.pallas_call(
        functools.partial(kernel, (rows, cols, chunks, per, 1, 2)),
        out_shape=jax.ShapeDtypeStruct((share_x, share_y, grid_z), f32),
        in_specs=[hbm, hbm, hbm, vmem, vmem, vmem],
        out_specs=vmem,
        scratch_shapes=[
            pltpu.VMEM(velocity.shape, f32),
            pltpu.VMEM(held.shape, bf16),
            pltpu.VMEM(t.shape, bf16),
            pltpu.VMEM((part_y // SUB, 2, grid_x * SUB, part_z), bf16),
            pltpu.VMEM((chunks, rows * per, part_y, part_z), f32),
            pltpu.VMEM((share_x, grid_y, part_z), f32),
            pltpu.VMEM((chunks, per, grid_y, part_z), f32),
            pltpu.VMEM((share_x, share_y, grid_z), f32),
            pltpu.VMEM((2 * per * share_y, grid_z), bf16),
            pltpu.VMEM((grid_x, 128), f32),
            pltpu.VMEM((grid_y, 128), f32),
            pltpu.SemaphoreType.DMA((4,)),
            pltpu.SemaphoreType.DMA((chunks,)),
            pltpu.SemaphoreType.DMA((chunks, per)),
            pltpu.SemaphoreType.DMA((chunks,)),
            pltpu.SemaphoreType.DMA((chunks, cols - 1)),
        ],
        compiler_params=pltpu.CompilerParams(
            collective_id=0, has_side_effects=True, vmem_limit_bytes=46 * 2**20
        ),
    )(velocity, jnp.asarray(held), jnp.asarray(np.ascontiguousarray(t)),
      symbol_x[None, :], symbol_y[None, :], symbol_z[None, :])


def fits(rows, cols, shape):
    grid_x, part_y, part_z = shape
    grid_z = part_z * cols
    held = 7 * grid_x * part_y * part_z * 4 + 4 * grid_z * grid_z + 4 * (grid_x * SUB) ** 2
    even = rows & (rows - 1) == 0 and cols & (cols - 1) == 0 and grid_x % (8 * rows) == 0
    return even and part_y % SUB == 0 and part_z % 128 == 0 and (part_y * rows) % (SUB * cols) == 0 and held < 54 * 2**20


def local(rows, cols, velocity, symbol_x, symbol_y, symbol_z):
    if fits(rows, cols, velocity.shape):
        return transformed(rows, cols, velocity, symbol_x, symbol_y, symbol_z)
    part_values = along_dim(velocity, 0)
    part_values = lax.all_to_all(part_values, "row", split_axis=0, concat_axis=1, tiled=True)
    pencil_values = along_dim(part_values, 1)
    pencil_values = lax.all_to_all(pencil_values, "col", split_axis=1, concat_axis=2, tiled=True)
    pencil_values = along_dim(pencil_values, 2)
    share_x = pencil_values.shape[0]
    part_x = lax.dynamic_slice_in_dim(symbol_x, lax.axis_index("row") * share_x, share_x)
    share_y = pencil_values.shape[1]
    part_y = lax.dynamic_slice_in_dim(symbol_y, lax.axis_index("col") * share_y, share_y)
    symbol = part_x[:, None, None] + part_y[None, :, None] + symbol_z[None, None, :]
    return pencil_values * ((1.0 - 0.2 * symbol) / (1.0 + 0.2 * symbol))


def solution(mesh):
    placed = (P(None, "row", "col"), P(), P(), P())
    return jax.shard_map(
        functools.partial(local, mesh.shape["row"], mesh.shape["col"]),
        mesh=mesh, in_specs=placed, out_specs=P("row", "col", None), check_vma=False,
    )
```

```python
import functools

import jax
import jax.numpy as jnp
import numpy as np
from jax import lax
from jax.experimental import pallas as pl
from jax.experimental.pallas import tpu as pltpu
from jax.sharding import PartitionSpec as P

SUB = 8
MESH = pl.DeviceIdType.MESH


def mode_table(count):
    rank = jnp.arange(count)
    angle = 2.0 * jnp.pi / count * (rank[:, None] * rank[None, :] % count).astype(jnp.float32)
    return (jnp.cos(angle) + jnp.sin(angle)) * count ** (-0.5)


def along_dim(values, dim):
    moved = jnp.tensordot(
        values, mode_table(values.shape[dim]), axes=([dim], [0]), precision=lax.Precision.HIGHEST
    )
    return jnp.moveaxis(moved, -1, dim)


def fixed_table(count):
    rank = np.arange(count)
    angle = 2.0 * np.pi / count * (rank[:, None] * rank[None, :] % count)
    return ((np.cos(angle) + np.sin(angle)) * count ** (-0.5)).astype(np.float32)


def halves(table):
    high = table.astype(jnp.bfloat16)
    low = (table - high.astype(np.float32)).astype(jnp.bfloat16)
    return high, low


def split(values):
    high = values.astype(jnp.bfloat16)
    low = (values - high.astype(jnp.float32)).astype(jnp.bfloat16)
    return high, low


def product(a, b):
    return jnp.dot(a, b, preferred_element_type=jnp.float32)


def flipped(index, mask):
    out = index
    bit = 1
    while bit <= mask:
        if mask & bit:
            out = out + bit * (1 - 2 * ((index // bit) % 2))
        bit *= 2
    return out


def kernel(
    dims, v_hbm, w_hbm, t_hbm, sx_ref, sy_ref, sz_ref, out_ref,
    v, w, t, v_parts, xs, rbuf, ybuf, zbuf, lhs, sx_col, sy_col,
    load_sem, row_send, row_recv, col_send, col_recv,
):
    rows, cols, chunks, per, ahead, lag = dims
    part_y, part_z = v.shape[1], v.shape[2]
    grid_x, grid_y = v.shape[0], rbuf.shape[1]
    share_y, grid_z = zbuf.shape[1], zbuf.shape[2]
    tiles, tile = t.shape[1], t.shape[3]
    r, c = lax.axis_index("row"), lax.axis_index("col")

    pieces = 4 if grid_x % (4 * SUB) == 0 else 1
    piece = grid_x // pieces
    load_v = [
        pltpu.make_async_copy(
            v_hbm.at[pl.ds(p * piece, piece)], v.at[pl.ds(p * piece, piece)], load_sem.at[3 + p]
        )
        for p in range(pieces)
    ]
    load_w = pltpu.make_async_copy(w_hbm.at[0], w.at[0], load_sem.at[1])
    load_rest = pltpu.make_async_copy(w_hbm.at[pl.ds(1, chunks - 1)], w.at[pl.ds(1, chunks - 1)], load_sem.at[2])
    load_t = pltpu.make_async_copy(t_hbm, t, load_sem.at[0])
    for load in load_v:
        load.start()
    load_w.start()

    row_masks = sorted(range(1, rows), key=lambda m: (-bin(m // 2).count("1"), m))
    row_peers = [flipped(r, m) for m in row_masks]
    col_peers = [flipped(c, m) for m in range(1, cols)]

    barrier = pltpu.get_barrier_semaphore()
    for s in row_peers:
        pl.semaphore_signal(barrier, inc=1, device_id=(s, c), device_id_type=MESH)
    for s in col_peers:
        pl.semaphore_signal(barrier, inc=1, device_id=(r, s), device_id_type=MESH)

    for ref, column in ((sx_ref, sx_col), (sy_ref, sy_col)):
        column[...] = jnp.broadcast_to(ref[...], (128, ref.shape[1])).T
    step = SUB * SUB

    def part_loop(i, carry):
        for g in range(part_y // SUB):
            block = v[pl.ds(i * SUB, SUB), g * SUB:(g + 1) * SUB, :].reshape(step, part_z)
            high, low = split(block)
            v_parts[g, 0, pl.ds(pl.multiple_of(i * step, step), step), :] = high
            v_parts[g, 1, pl.ds(pl.multiple_of(i * step, step), step), :] = low
        return carry

    for p in range(pieces):
        load_v[p].wait()
        lax.fori_loop(p * piece // SUB, (p + 1) * piece // SUB, part_loop, 0)
    load_w.wait()
    load_rest.start()
    load_t.start()
    pl.semaphore_wait(barrier, len(row_peers) + len(col_peers))

    def x_stage(k):
        m, depth = rows * per * SUB, grid_x * SUB
        for g in range(part_y // SUB):
            both = product(w[k, :2 * m, :depth], v_parts[g, 0])
            sums = both[:m] + both[m:] + product(w[k, :m, :depth], v_parts[g, 1])
            xs[k, :, g * SUB:(g + 1) * SUB, :] = sums.reshape(rows * per, SUB, part_z)

    def own_rows():
        return pl.ds(pl.multiple_of(r * part_y, SUB), part_y)

    def row_stage(k):
        for i in range(per):
            for s in row_peers:
                pltpu.make_async_remote_copy(
                    src_ref=xs.at[k, s * per + i],
                    dst_ref=rbuf.at[k * per + i, own_rows(), :],
                    send_sem=row_send.at[k], recv_sem=row_recv.at[k, i],
                    device_id=(s, c), device_id_type=MESH,
                ).start()
        rbuf[pl.ds(k * per, per), own_rows(), :] = xs[k, pl.ds(r * per, per)]

    def y_stage(k):
        for i in range(per):
            came = rbuf.at[k * per + i, pl.ds(0, grid_y - part_y), :]
            pltpu.make_async_copy(came, came, row_recv.at[k, i]).wait()
            high, low = split(rbuf[k * per + i])
            both = product(w[0, :2 * grid_y, grid_x * SUB:], high)
            ybuf[k, i] = both[:grid_y] + both[grid_y:] + product(w[0, :grid_y, grid_x * SUB:], low)
            for m, s in enumerate(col_peers):
                pltpu.make_async_remote_copy(
                    src_ref=ybuf.at[k, i, pl.ds(pl.multiple_of(s * share_y, SUB), share_y), :],
                    dst_ref=zbuf.at[k * per + i, :, pl.ds(pl.multiple_of(c * part_z, 128), part_z)],
                    send_sem=col_send.at[k], recv_sem=col_recv.at[k, m],
                    device_id=(r, s), device_id_type=MESH,
                ).start()
        zbuf[pl.ds(k * per, per), :, pl.ds(pl.multiple_of(c * part_z, 128), part_z)] = (
            ybuf[k, :, pl.ds(pl.multiple_of(c * share_y, SUB), share_y), :]
        )

    def col_wait(k, m):
        came = zbuf.at[pl.ds(k * per, per), :, pl.ds(0, part_z)]
        pltpu.make_async_copy(came, came, col_recv.at[k, m]).wait()

    def scaled(k, n, sums):
        y_part = sy_col[pl.ds(pl.multiple_of(c * share_y, SUB), share_y), :]
        z_part = sz_ref[:, pl.ds(pl.multiple_of(n * tile, tile), tile)]
        plane = jnp.concatenate([y_part] * (tile // 128), axis=1) + z_part
        for i in range(per):
            x_part = sx_col[pl.ds(r * chunks * per + k * per + i, 1), :]
            symbol = jnp.concatenate([x_part] * (tile // 128), axis=1) + plane
            factor = (1.0 - 0.2 * symbol) / (1.0 + 0.2 * symbol)
            out_ref[k * per + i, :, pl.ds(pl.multiple_of(n * tile, tile), tile)] = (
                sums[i * share_y:(i + 1) * share_y] * factor
            )

    size = per * share_y

    def z_stage(k):
        for m in range(len(col_peers)):
            col_wait(k, m)
        high, low = split(zbuf[pl.ds(k * per, per)].reshape(size, grid_z))
        lhs[:size] = high
        lhs[size:] = low

        def tile_loop(n, carry):
            both = product(lhs[...], t[0, n])
            scaled(k, n, both[:size] + both[size:] + product(lhs[:size], t[1, n]))
            return carry

        lax.fori_loop(0, tiles, tile_loop, 0)

    def last_z_stage(k):
        for m, s in enumerate([c] + col_peers):
            if m > 0:
                col_wait(k, m - 1)
            span = pl.ds(pl.multiple_of(s * part_z, 128), part_z)
            high, low = split(zbuf[pl.ds(k * per, per), :, span].reshape(size, part_z))
            lhs[:size, :part_z] = high
            lhs[size:, :part_z] = low

            def tile_loop(n, carry):
                both = product(lhs[:, :part_z], t[0, n, span, :])
                sums = both[:size] + both[size:] + product(lhs[:size, :part_z], t[1, n, span, :])
                at = pl.ds(pl.multiple_of(n * tile, tile), tile)
                if m > 0:
                    sums = sums + out_ref[pl.ds(k * per, per), :, at].reshape(size, tile)
                if m < len(col_peers):
                    out_ref[pl.ds(k * per, per), :, at] = sums.reshape(per, share_y, tile)
                else:
                    scaled(k, n, sums)
                return carry

            lax.fori_loop(0, tiles, tile_loop, 0)

    def loop(k, carry):
        @pl.when(k == 1)
        def _():
            load_rest.wait()

        @pl.when(k < chunks)
        def _():
            x_stage(k)
            row_stage(k)

        @pl.when((k >= ahead) & (k < chunks + ahead))
        def _():
            y_stage(k - ahead)

        @pl.when(k == ahead + lag)
        def _():
            load_t.wait()

        @pl.when(k >= ahead + lag)
        def _():
            z_stage(k - ahead - lag)

        return carry

    lax.fori_loop(0, chunks + ahead + lag - 1, loop, 0)
    last_z_stage(chunks - 1)

    def drain(k, carry):
        sent = rbuf.at[pl.ds(k * per, per), pl.ds(0, grid_y - part_y), :]
        pltpu.make_async_copy(sent, sent, row_send.at[k]).wait()
        sent = zbuf.at[pl.ds(k * per, per), :, pl.ds(0, grid_z - part_z)]
        pltpu.make_async_copy(sent, sent, col_send.at[k]).wait()
        return carry

    lax.fori_loop(0, chunks, drain, 0)


def transformed(rows, cols, velocity, symbol_x, symbol_y, symbol_z):
    grid_x, part_y, part_z = velocity.shape
    grid_y, grid_z = part_y * rows, part_z * cols
    share_x, share_y = grid_x // rows, grid_y // cols
    chunks = min(8, share_x)
    per = share_x // chunks
    tile = 256
    hx, hy, hz = fixed_table(grid_x), fixed_table(grid_y), fixed_table(grid_z)
    order = np.arange(grid_x).reshape(rows, chunks, per).transpose(1, 0, 2).reshape(chunks, rows * per)
    w = np.stack([np.kron(hx[o], np.eye(SUB, dtype=np.float32)) for o in order])
    w = np.concatenate(halves(w), axis=1)
    h = np.concatenate(halves(hy), axis=0)
    t = np.stack(halves(hz)).reshape(2, grid_z, grid_z // tile, tile).transpose(0, 2, 1, 3)
    held = np.zeros((chunks, max(w.shape[1], h.shape[0]), w.shape[2] + h.shape[1]), w.dtype)
    held[:, :w.shape[1], :w.shape[2]] = w
    held[0, :h.shape[0], w.shape[2]:] = h
    f32, bf16 = jnp.float32, jnp.bfloat16
    hbm = pl.BlockSpec(memory_space=pltpu.HBM)
    vmem = pl.BlockSpec(memory_space=pltpu.VMEM)
    return pl.pallas_call(
        functools.partial(kernel, (rows, cols, chunks, per, 1, 2)),
        out_shape=jax.ShapeDtypeStruct((share_x, share_y, grid_z), f32),
        in_specs=[hbm, hbm, hbm, vmem, vmem, vmem],
        out_specs=vmem,
        scratch_shapes=[
            pltpu.VMEM(velocity.shape, f32),
            pltpu.VMEM(held.shape, bf16),
            pltpu.VMEM(t.shape, bf16),
            pltpu.VMEM((part_y // SUB, 2, grid_x * SUB, part_z), bf16),
            pltpu.VMEM((chunks, rows * per, part_y, part_z), f32),
            pltpu.VMEM((share_x, grid_y, part_z), f32),
            pltpu.VMEM((chunks, per, grid_y, part_z), f32),
            pltpu.VMEM((share_x, share_y, grid_z), f32),
            pltpu.VMEM((2 * per * share_y, grid_z), bf16),
            pltpu.VMEM((grid_x, 128), f32),
            pltpu.VMEM((grid_y, 128), f32),
            pltpu.SemaphoreType.DMA((7,)),
            pltpu.SemaphoreType.DMA((chunks,)),
            pltpu.SemaphoreType.DMA((chunks, per)),
            pltpu.SemaphoreType.DMA((chunks,)),
            pltpu.SemaphoreType.DMA((chunks, cols - 1)),
        ],
        compiler_params=pltpu.CompilerParams(
            collective_id=0, has_side_effects=True, vmem_limit_bytes=46 * 2**20
        ),
    )(velocity, jnp.asarray(held), jnp.asarray(np.ascontiguousarray(t)),
      symbol_x[None, :], symbol_y[None, :], symbol_z[None, :])


def fits(rows, cols, shape):
    grid_x, part_y, part_z = shape
    grid_z = part_z * cols
    held = 7 * grid_x * part_y * part_z * 4 + 4 * grid_z * grid_z + 4 * (grid_x * SUB) ** 2
    even = rows & (rows - 1) == 0 and cols & (cols - 1) == 0 and grid_x % (8 * rows) == 0
    return even and part_y % SUB == 0 and part_z % 128 == 0 and (part_y * rows) % (SUB * cols) == 0 and held < 54 * 2**20


def local(rows, cols, velocity, symbol_x, symbol_y, symbol_z):
    if fits(rows, cols, velocity.shape):
        return transformed(rows, cols, velocity, symbol_x, symbol_y, symbol_z)
    part_values = along_dim(velocity, 0)
    part_values = lax.all_to_all(part_values, "row", split_axis=0, concat_axis=1, tiled=True)
    pencil_values = along_dim(part_values, 1)
    pencil_values = lax.all_to_all(pencil_values, "col", split_axis=1, concat_axis=2, tiled=True)
    pencil_values = along_dim(pencil_values, 2)
    share_x = pencil_values.shape[0]
    part_x = lax.dynamic_slice_in_dim(symbol_x, lax.axis_index("row") * share_x, share_x)
    share_y = pencil_values.shape[1]
    part_y = lax.dynamic_slice_in_dim(symbol_y, lax.axis_index("col") * share_y, share_y)
    symbol = part_x[:, None, None] + part_y[None, :, None] + symbol_z[None, None, :]
    return pencil_values * ((1.0 - 0.2 * symbol) / (1.0 + 0.2 * symbol))


def solution(mesh):
    placed = (P(None, "row", "col"), P(), P(), P())
    return jax.shard_map(
        functools.partial(local, mesh.shape["row"], mesh.shape["col"]),
        mesh=mesh, in_specs=placed, out_specs=P("row", "col", None), check_vma=False,
    )
```
